32 devices in a mesh: ab: 4 (over x, core), kl: 4 (over z), ij: 2 (over y).
Axes of the slice: x: 2, y: 2, z: 4, core: 2. Of those that a mesh axis runs over, the one named last changes fastest.
Arguments:
- amplitudes: bfloat16 [2048, 8192], P('ab', ('kl', 'ij')), may hold values from -6 to 6
- integrals: bfloat16 [8192, 8192], P(('kl', 'ab'), 'ij'), may hold values from -0.0625 to 0.0625
Outputs:
- ladder: float32 [2048, 8192], P('ab', ('ij', 'kl'))
The draws below stay inside these ranges and needn't reach their ends.
All inputs are finite; a program needn't handle non-finite values.
Results may differ from the reference program's by a relative error of at most 0.0003.
Values may be sent and summed in bfloat16 or wider, within the bound.
A program may use at most 64 MiB of HBM per device.

```python
import jax
import jax.numpy as jnp
from jax import lax

PAIRS = 8128
PADDED = 8192
VPAIRS = 2048


def block_scale(stream_key, extent, cuts, smallest, high):
    gain = 1.0
    for dim, shards_of in cuts:
        heights = jax.random.uniform(jax.random.fold_in(jax.random.fold_in(stream_key, 6), dim), (shards_of,), jnp.float32, smallest / len(cuts), high / len(cuts))
        gain = gain * jnp.repeat(jnp.exp(heights), extent[dim] // shards_of).reshape((-1,) + (1,) * (len(extent) - 1 - dim))
    return gain


def noise(rng, extent, spread, most, pieces=(), held_as=jnp.bfloat16):
    entries = jax.random.normal(rng, extent, jnp.float32) * spread
    if len(pieces) > 0:
        entries = block_scale(rng, extent, pieces, -0.22, 0.18) * entries
    return jnp.clip(entries, min=-most, max=most).astype(held_as)


def setup_inputs(seed: int = 0) -> dict:
    arg_keys = jax.random.split(jax.random.key(seed), 3)
    amplitudes = noise(arg_keys[0], (VPAIRS, PADDED), 1.0, 6.0, ((0, 4), (1, 8)))
    integrals = noise(arg_keys[1], (PADDED, PADDED), PAIRS ** -0.5, 0.0625, ((0, 16), (1, 2)))
    return {"amplitudes": amplitudes, "integrals": integrals}


def reference(amplitudes, integrals):
    keep = jnp.arange(PADDED) < PAIRS
    left = jnp.where(keep[None, :], amplitudes.astype(jnp.float32), jnp.float32(0.0))
    full = jnp.dot(left, integrals.astype(jnp.float32), precision=lax.Precision.HIGHEST)
    return jnp.where(keep[None, :], full, jnp.float32(0.0))
```

```python
import functools
import math

import jax
import jax.numpy as jnp
from jax import lax
from jax.experimental import pallas as pl
from jax.experimental.pallas import tpu as pltpu
from jax.sharding import PartitionSpec as P

PAIRS = 8128
MESH = pl.DeviceIdType.MESH
CHUNK = 256
TOP = 2.0**7.75
HEAD = 16


def visit_order(n):
    return [sorted(range(n), key=lambda d: (-abs(d - k), d > k)) for k in range(n)]


def encode_into(buf, slot, value):
    peak = jnp.max(jnp.abs(value), axis=0, keepdims=True)
    held = jnp.maximum(peak, 1e-30).astype(jnp.bfloat16)
    scaled = value * (TOP / held.astype(jnp.float32))
    p2 = scaled * scaled
    p4 = p2 * p2
    p8 = p4 * p4
    p16 = p8 * p8
    rows = value.shape[0]
    buf[slot, pl.ds(0, rows), :] = jnp.where(scaled < 0, -p16, p16).astype(jnp.bfloat16)
    buf[slot, pl.ds(rows, HEAD), :] = jnp.broadcast_to(held, (HEAD, held.shape[1]))


def decode(buf, slot, rows):
    code = buf[slot, pl.ds(0, rows), :].astype(jnp.float32)
    held = buf[slot, pl.ds(rows, HEAD), :].astype(jnp.float32)[:1]
    size = jnp.sqrt(jnp.sqrt(jnp.sqrt(jnp.sqrt(jnp.abs(code)))))
    return jnp.where(code < 0, -size, size) * (held * (1.0 / TOP))


def kernel(n_ab, n_kl, n_ij, w, a_ref, b_ref, o_ref, ag, bg, lb, rb, sb, acc,
           a_s, a_r, x_s, x_r, f_s, f_r, c_s, c_r, l_r, z_s, zl_r, zr_r):
    ab, kl, ij = lax.axis_index("ab"), lax.axis_index("kl"), lax.axis_index("ij")
    n_pair = n_ab // 2
    pair, core = ab // 2, ab % 2
    sib = ab + 1 - 2 * core
    m, ka = a_ref.shape
    r = b_ref.shape[0]
    width = o_ref.shape[1]
    per = width // w
    chunks = n_kl * per
    orders = visit_order(n_kl)

    def peer(o):
        return ((pair + o) % n_pair) * 2 + core

    def source(o):
        return ((pair + n_pair - o) % n_pair) * 2 + core

    def dest_of(i):
        t = i // per
        d = jnp.int32(0)
        for k in range(n_kl):
            for u in range(n_kl):
                d = jnp.where((kl == k) & (t == u), orders[k][u], d)
        return d

    def cols_of(i):
        return pl.ds(pl.multiple_of(dest_of(i) * width + (i % per) * w, w), w)

    def rows_of(dev):
        return pl.ds(pl.multiple_of(dev * r, r), r)

    barrier = pltpu.get_barrier_semaphore()

    def greet(dev):
        pl.semaphore_signal(barrier, inc=1, device_id=dev, device_id_type=MESH)

    for o in range(1, n_pair):
        greet((peer(o), kl, ij))
    greet((sib, kl, ij))
    for o in range(1, n_ij):
        greet((ab, kl, (ij + o) % n_ij))

    @pl.when(kl > 0)
    def _():
        greet((ab, kl - 1, ij))

    @pl.when(kl < n_kl - 1)
    def _():
        greet((ab, kl + 1, ij))

    lines = (kl > 0).astype(jnp.int32) + (kl < n_kl - 1).astype(jnp.int32)
    pl.semaphore_wait(barrier, n_pair + n_ij - 1 + lines)

    def a_copy(o):
        return pltpu.make_async_remote_copy(
            a_ref, ag.at[ij], a_s.at[o - 1], a_r.at[o - 1],
            device_id=(ab, kl, (ij + o) % n_ij), device_id_type=MESH)

    def x_copy(i, o):
        return pltpu.make_async_remote_copy(
            b_ref.at[:, cols_of(i)], bg.at[i, rows_of(ab), :],
            x_s.at[i, o - 1], x_r.at[i, o - 1],
            device_id=(peer(o), kl, ij), device_id_type=MESH)

    def f_copy(i, o):
        there = bg.at[i, rows_of(source(o)), :]
        return pltpu.make_async_remote_copy(
            there, there, f_s.at[i, o - 1], f_r.at[i, o - 1],
            device_id=(sib, kl, ij), device_id_type=MESH)

    def c_copy(i):
        return pltpu.make_async_remote_copy(
            b_ref.at[:, cols_of(i)], bg.at[i, rows_of(ab), :], c_s.at[i], c_r.at[i],
            device_id=(sib, kl, ij), device_id_type=MESH)

    def l_copy(i):
        return pltpu.make_async_copy(
            b_ref.at[:, cols_of(i)], bg.at[i, rows_of(ab), :], l_r.at[i])

    def z_copy(i, slot, up):
        box, sem = (lb, zl_r) if up else (rb, zr_r)
        return pltpu.make_async_remote_copy(
            sb.at[i], box.at[slot], z_s.at[i], sem.at[slot],
            device_id=(ab, kl + 1 if up else kl - 1, ij), device_id_type=MESH)

    for o in range(1, n_ij):
        a_copy(o).start()

    def begin(i, carry):
        for o in range(1, n_pair):
            x_copy(i, o).start()
        c_copy(i).start()
        l_copy(i).start()
        return carry

    lax.fori_loop(0, chunks, begin, 0)

    ag[ij] = a_ref[...]
    for o in range(1, n_ij):
        a_copy(o).wait_recv()
    for j in range(n_ij):
        first = kl * (ka * n_ij) + j * ka

        @pl.when(first + ka > PAIRS)
        def _():
            ids = first + lax.broadcasted_iota(jnp.int32, (m, ka), 1)
            ag[j] = jnp.where(ids < PAIRS, ag[j].astype(jnp.float32), 0.0).astype(jnp.bfloat16)

    def step(i, carry):
        for o in range(1, n_pair):
            x_copy(i, o).wait_recv()
            f_copy(i, o).start()
        l_copy(i).wait()
        c_copy(i).wait_recv()
        for o in range(1, n_pair):
            f_copy(i, o).wait_recv()
        total = jnp.dot(ag[0], bg[i, pl.ds(0, ka), :], preferred_element_type=jnp.float32)
        for j in range(1, n_ij):
            total += jnp.dot(ag[j], bg[i, pl.ds(j * ka, ka), :], preferred_element_type=jnp.float32)
        acc[...] = total
        d = dest_of(i)
        slot = d * per + i % per

        @pl.when((d >= kl) & (kl > 0))
        def _():
            z_copy(i, slot, True).wait_recv()
            acc[...] += decode(lb, slot, m)

        @pl.when((d <= kl) & (kl < n_kl - 1))
        def _():
            z_copy(i, slot, False).wait_recv()
            acc[...] += decode(rb, slot, m)

        @pl.when(d == kl)
        def _():
            first = pl.multiple_of((i % per) * w, w)
            ids = (ij * n_kl + kl) * width + first + lax.broadcasted_iota(jnp.int32, (m, w), 1)
            o_ref[:, pl.ds(first, w)] = jnp.where(ids < PAIRS, acc[...], 0.0)

        @pl.when(d != kl)
        def _():
            encode_into(sb, i, acc[...])

        @pl.when(d > kl)
        def _():
            z_copy(i, slot, True).start()

        @pl.when(d < kl)
        def _():
            z_copy(i, slot, False).start()

        return carry

    lax.fori_loop(0, chunks, step, 0)

    for o in range(1, n_ij):
        a_copy(o).wait_send()

    def drain(i, carry):
        for o in range(1, n_pair):
            x_copy(i, o).wait_send()
            f_copy(i, o).wait_send()
        c_copy(i).wait_send()

        @pl.when(dest_of(i) > kl)
        def _():
            z_copy(i, 0, True).wait_send()

        @pl.when(dest_of(i) < kl)
        def _():
            z_copy(i, 0, False).wait_send()

        return carry

    lax.fori_loop(0, chunks, drain, 0)


def per_device(n_ab, n_kl, n_ij, amplitudes, integrals):
    m, ka = amplitudes.shape
    r, n = integrals.shape
    width = n // n_kl
    w = math.gcd(CHUNK, width)
    chunks = n // w
    others = max(n_ab // 2 - 1, 1)
    mail = pltpu.VMEM((chunks, m + HEAD, w), jnp.bfloat16)
    dma = pltpu.SemaphoreType.DMA
    return pl.pallas_call(
        functools.partial(kernel, n_ab, n_kl, n_ij, w),
        out_shape=jax.ShapeDtypeStruct((m, width), jnp.float32),
        in_specs=[pl.BlockSpec(memory_space=pltpu.VMEM), pl.BlockSpec(memory_space=pl.ANY)],
        out_specs=pl.BlockSpec(memory_space=pltpu.VMEM),
        scratch_shapes=[
            pltpu.VMEM((n_ij, m, ka), jnp.bfloat16),
            pltpu.VMEM((chunks, n_ab * r, w), jnp.bfloat16),
            mail, mail, mail,
            pltpu.VMEM((m, w), jnp.float32),
            dma((max(n_ij - 1, 1),)), dma((max(n_ij - 1, 1),)),
            dma((chunks, others)), dma((chunks, others)),
            dma((chunks, others)), dma((chunks, others)),
            dma((chunks,)), dma((chunks,)), dma((chunks,)),
            dma((chunks,)), dma((chunks,)), dma((chunks,)),
        ],
        compiler_params=pltpu.CompilerParams(
            collective_id=0, has_side_effects=True, vmem_limit_bytes=56 * 2**20),
    )(amplitudes, integrals)


def solution(mesh):
    sizes = [mesh.shape[name] for name in ("ab", "kl", "ij")]
    in_specs = (P("ab", ("kl", "ij")), P(("kl", "ab"), "ij"))
    out_specs = P("ab", ("ij", "kl"))
    return jax.shard_map(
        functools.partial(per_device, *sizes), mesh=mesh, in_specs=in_specs,
        out_specs=out_specs, check_vma=False
    )
```

```python
import functools
import math

import jax
import jax.numpy as jnp
from jax import lax
from jax.experimental import pallas as pl
from jax.experimental.pallas import tpu as pltpu
from jax.sharding import PartitionSpec as P

PAIRS = 8128
MESH = pl.DeviceIdType.MESH
CHUNK = 256
TOP = 2.0**7.75
HEAD = 16
PIECES = 2


def visit_order(n):
    return [sorted(range(n), key=lambda d: (-abs(d - k), d > k)) for k in range(n)]


def encode_into(buf, slot, q, value):
    peak = jnp.max(jnp.abs(value), axis=0, keepdims=True)
    held = jnp.maximum(peak, 1e-30).astype(jnp.bfloat16)
    scaled = value * (TOP / held.astype(jnp.float32))
    p2 = scaled * scaled
    p4 = p2 * p2
    p8 = p4 * p4
    p16 = p8 * p8
    rows = value.shape[0]
    buf[slot, q, pl.ds(0, rows), :] = jnp.where(scaled < 0, -p16, p16).astype(jnp.bfloat16)
    buf[slot, q, pl.ds(rows, HEAD), :] = jnp.broadcast_to(held, (HEAD, held.shape[1]))


def decode(buf, slot, q, rows):
    code = buf[slot, q, pl.ds(0, rows), :].astype(jnp.float32)
    held = buf[slot, q, pl.ds(rows, HEAD), :].astype(jnp.float32)[:1]
    size = jnp.sqrt(jnp.sqrt(jnp.sqrt(jnp.sqrt(jnp.abs(code)))))
    return jnp.where(code < 0, -size, size) * (held * (1.0 / TOP))


def kernel(n_ab, n_kl, n_ij, w, pieces, a_ref, b_ref, o_ref, ag, bg, lb, rb, sb, acc,
           a_s, a_r, x_s, x_r, f_s, f_r, c_s, c_r, l_r, z_s, zl_r, zr_r):
    ab, kl, ij = lax.axis_index("ab"), lax.axis_index("kl"), lax.axis_index("ij")
    n_pair = n_ab // 2
    pair, core = ab // 2, ab % 2
    sib = ab + 1 - 2 * core
    m, ka = a_ref.shape
    r = b_ref.shape[0]
    width = o_ref.shape[1]
    per = width // w
    chunks = n_kl * per
    orders = visit_order(n_kl)
    mp = m // pieces
    lead = min(pieces, chunks)

    def peer(o):
        return ((pair + o) % n_pair) * 2 + core

    def source(o):
        return ((pair + n_pair - o) % n_pair) * 2 + core

    def dest_of(i):
        t = i // per
        d = jnp.int32(0)
        for k in range(n_kl):
            for u in range(n_kl):
                d = jnp.where((kl == k) & (t == u), orders[k][u], d)
        return d

    def cols_of(i):
        return pl.ds(pl.multiple_of(dest_of(i) * width + (i % per) * w, w), w)

    def rows_of(dev):
        return pl.ds(pl.multiple_of(dev * r, r), r)

    barrier = pltpu.get_barrier_semaphore()

    def greet(dev):
        pl.semaphore_signal(barrier, inc=1, device_id=dev, device_id_type=MESH)

    for o in range(1, n_pair):
        greet((peer(o), kl, ij))
    greet((sib, kl, ij))
    for o in range(1, n_ij):
        greet((ab, kl, (ij + o) % n_ij))

    @pl.when(kl > 0)
    def _():
        greet((ab, kl - 1, ij))

    @pl.when(kl < n_kl - 1)
    def _():
        greet((ab, kl + 1, ij))

    lines = (kl > 0).astype(jnp.int32) + (kl < n_kl - 1).astype(jnp.int32)
    pl.semaphore_wait(barrier, n_pair + n_ij - 1 + lines)

    def slab(q):
        return pl.ds(pl.multiple_of(q * mp, mp), mp)

    def a_copy(o, q):
        return pltpu.make_async_remote_copy(
            a_ref.at[slab(q), :], ag.at[ij, slab(q), :], a_s.at[o - 1, q], a_r.at[o - 1, q],
            device_id=(ab, kl, (ij + o) % n_ij), device_id_type=MESH)

    def x_copy(i, o):
        return pltpu.make_async_remote_copy(
            b_ref.at[:, cols_of(i)], bg.at[i, rows_of(ab), :],
            x_s.at[i, o - 1], x_r.at[i, o - 1],
            device_id=(peer(o), kl, ij), device_id_type=MESH)

    def f_copy(i, o):
        there = bg.at[i, rows_of(source(o)), :]
        return pltpu.make_async_remote_copy(
            there, there, f_s.at[i, o - 1], f_r.at[i, o - 1],
            device_id=(sib, kl, ij), device_id_type=MESH)

    def c_copy(i):
        return pltpu.make_async_remote_copy(
            b_ref.at[:, cols_of(i)], bg.at[i, rows_of(ab), :], c_s.at[i], c_r.at[i],
            device_id=(sib, kl, ij), device_id_type=MESH)

    def l_copy(i):
        return pltpu.make_async_copy(
            b_ref.at[:, cols_of(i)], bg.at[i, rows_of(ab), :], l_r.at[i])

    def z_copy(i, q, slot, up):
        box, sem = (lb, zl_r) if up else (rb, zr_r)
        return pltpu.make_async_remote_copy(
            sb.at[i, q], box.at[slot, q], z_s.at[i, q], sem.at[slot, q],
            device_id=(ab, kl + 1 if up else kl - 1, ij), device_id_type=MESH)

    for q in range(pieces):
        for o in range(1, n_ij):
            a_copy(o, q).start()

    def begin(i, carry):
        for o in range(1, n_pair):
            x_copy(i, o).start()
        c_copy(i).start()
        l_copy(i).start()
        return carry

    lax.fori_loop(0, chunks, begin, 0)

    def take_chunk(i):
        for o in range(1, n_pair):
            x_copy(i, o).wait_recv()
            f_copy(i, o).start()
        l_copy(i).wait()
        c_copy(i).wait_recv()
        for o in range(1, n_pair):
            f_copy(i, o).wait_recv()

    def take_piece(q):
        ag[ij, slab(q), :] = a_ref[slab(q), :]
        for o in range(1, n_ij):
            a_copy(o, q).wait_recv()
        for j in range(n_ij):
            first = kl * (ka * n_ij) + j * ka

            @pl.when(first + ka > PAIRS)
            def _():
                ids = first + lax.broadcasted_iota(jnp.int32, (mp, ka), 1)
                held = ag[j, slab(q), :].astype(jnp.float32)
                ag[j, slab(q), :] = jnp.where(ids < PAIRS, held, 0.0).astype(jnp.bfloat16)

    def unit(u):
        v = jnp.int32(0)
        for k in range(1, lead):
            v += (u >= k * k).astype(jnp.int32)
        left = u - v * v
        own = left <= v
        rest = u - lead * lead
        early = u < lead * lead
        i = jnp.where(early, jnp.where(own, v, left - v - 1), lead + rest // pieces)
        q = jnp.where(early, jnp.where(own, left, v), rest % pieces)
        return i, q

    def step(u, carry):
        i, q = unit(u)

        @pl.when(q == 0)
        def _():
            take_chunk(i)

        @pl.when(i == q)
        def _():
            take_piece(q)

        acc[...] = sum(
            jnp.dot(ag[j, slab(q), :], bg[i, pl.ds(j * ka, ka), :],
                    preferred_element_type=jnp.float32)
            for j in range(n_ij))
        d = dest_of(i)
        slot = d * per + i % per

        @pl.when((d >= kl) & (kl > 0))
        def _():
            z_copy(i, q, slot, True).wait_recv()
            acc[...] += decode(lb, slot, q, mp)

        @pl.when((d <= kl) & (kl < n_kl - 1))
        def _():
            z_copy(i, q, slot, False).wait_recv()
            acc[...] += decode(rb, slot, q, mp)

        @pl.when(d == kl)
        def _():
            first = pl.multiple_of((i % per) * w, w)
            ids = (ij * n_kl + kl) * width + first + lax.broadcasted_iota(jnp.int32, (mp, w), 1)
            o_ref[slab(q), pl.ds(first, w)] = jnp.where(ids < PAIRS, acc[...], 0.0)

        @pl.when(d != kl)
        def _():
            encode_into(sb, i, q, acc[...])

        @pl.when(d > kl)
        def _():
            z_copy(i, q, slot, True).start()

        @pl.when(d < kl)
        def _():
            z_copy(i, q, slot, False).start()

        return carry

    lax.fori_loop(0, chunks * pieces, step, 0)

    for q in range(pieces):
        for o in range(1, n_ij):
            a_copy(o, q).wait_send()

    def drain(i, carry):
        for o in range(1, n_pair):
            x_copy(i, o).wait_send()
            f_copy(i, o).wait_send()
        c_copy(i).wait_send()
        for q in range(pieces):
            @pl.when(dest_of(i) > kl)
            def _():
                z_copy(i, q, 0, True).wait_send()

            @pl.when(dest_of(i) < kl)
            def _():
                z_copy(i, q, 0, False).wait_send()

        return carry

    lax.fori_loop(0, chunks, drain, 0)


def per_device(n_ab, n_kl, n_ij, amplitudes, integrals):
    m, ka = amplitudes.shape
    r, n = integrals.shape
    width = n // n_kl
    w = math.gcd(CHUNK, width)
    chunks = n // w
    others = max(n_ab // 2 - 1, 1)
    pieces = min(PIECES, chunks, m // 16)
    mail = pltpu.VMEM((chunks, pieces, m // pieces + HEAD, w), jnp.bfloat16)
    dma = pltpu.SemaphoreType.DMA
    return pl.pallas_call(
        functools.partial(kernel, n_ab, n_kl, n_ij, w, pieces),
        out_shape=jax.ShapeDtypeStruct((m, width), jnp.float32),
        in_specs=[pl.BlockSpec(memory_space=pltpu.VMEM), pl.BlockSpec(memory_space=pl.ANY)],
        out_specs=pl.BlockSpec(memory_space=pltpu.VMEM),
        scratch_shapes=[
            pltpu.VMEM((n_ij, m, ka), jnp.bfloat16),
            pltpu.VMEM((chunks, n_ab * r, w), jnp.bfloat16),
            mail, mail, mail,
            pltpu.VMEM((m // pieces, w), jnp.float32),
            dma((max(n_ij - 1, 1), pieces)), dma((max(n_ij - 1, 1), pieces)),
            dma((chunks, others)), dma((chunks, others)),
            dma((chunks, others)), dma((chunks, others)),
            dma((chunks,)), dma((chunks,)), dma((chunks,)),
            dma((chunks, pieces)), dma((chunks, pieces)), dma((chunks, pieces)),
        ],
        compiler_params=pltpu.CompilerParams(
            collective_id=0, has_side_effects=True, vmem_limit_bytes=56 * 2**20),
    )(amplitudes, integrals)


def solution(mesh):
    sizes = [mesh.shape[name] for name in ("ab", "kl", "ij")]
    in_specs = (P("ab", ("kl", "ij")), P(("kl", "ab"), "ij"))
    out_specs = P("ab", ("ij", "kl"))
    return jax.shard_map(
        functools.partial(per_device, *sizes), mesh=mesh, in_specs=in_specs,
        out_specs=out_specs, check_vma=False
    )
```
